32 devices in a mesh: seq: 8 (over y, x, core), head: 4 (over z).
Axes of the slice: x: 2, y: 2, z: 4, core: 2. Of those that a mesh axis runs over, the one named last changes fastest.
Arguments:
- query: bfloat16 [2, 1024, 4096], P(None, 'seq', 'head'), may hold values from -5 to 5
- keys: bfloat16 [2, 1024, 1024], P(None, 'seq', 'head'), may hold values from -5 to 5
- values: bfloat16 [2, 1024, 1024], P(None, 'seq', 'head'), may hold values from -12 to 12
- norm_gain: float32 [4096], P('head'), may hold values from 0.25 to 1.75
- in_b: bfloat16 [2048, 128], P('seq'), may hold values from -0.25 to 0.25
- out_c: bfloat16 [2048, 128], P('seq'), may hold values from -0.25 to 0.25
- step: float32 [64, 2048], P('head', 'seq'), may hold values from 0.2 to 1
- log_decay: float32 [64, 2048], P('head', 'seq'), may hold values from -2 to 0
- skip: float32 [64], P('head'), may hold values from 0.5 to 1.5
Outputs:
- mixed: bfloat16 [2048, 4096], P('seq', 'head')
The draws below stay inside these ranges and needn't reach their ends.
All inputs are finite; a program needn't handle non-finite values.
Results may differ from the reference program's by a relative error of at most 0.012.
Values may be sent and summed in bfloat16 or wider, within the bound.
A program may use at most 128 MiB of HBM per device.

```python
import math
import jax
import jax.numpy as jnp
from jax import lax

HEADS = 32
KVH = 8
HDIM = 128
SHEADS = 64
SDIM = 64
STATE = 128
SPAN = 256
TOKEN_COUNT = 2048
BLK = 128
WIN = 256


def qk_pair(key):
    baseline_rate = jax.random.fold_in(key, 11)
    key_query, key_keys = jax.random.split(baseline_rate, 2)
    queries = jnp.clip(jax.random.normal(key_query, (TOKEN_COUNT, HEADS * HDIM), jnp.float32), -4.0, 4.0)
    keyvals = jnp.clip(jax.random.normal(key_keys, (TOKEN_COUNT, KVH * HDIM), jnp.float32), -4.0, 4.0)
    queries = queries.reshape(2, TOKEN_COUNT // 2, HEADS * HDIM).astype(jnp.bfloat16)
    keyvals = keyvals.reshape(2, TOKEN_COUNT // 2, KVH * HDIM).astype(jnp.bfloat16)
    return (queries, keyvals)


def draw_query(key, part):
    return qk_pair(key)[0]


def draw_keys(key, part):
    return qk_pair(key)[1]


def draw_values(key, part):
    baseline_rate = jax.random.fold_in(key, 23)
    head_scale = 3.0 ** (jnp.arange(KVH, dtype=jnp.float32) / (KVH - 1))
    raw_values = jnp.clip(jax.random.normal(baseline_rate, (TOKEN_COUNT, KVH, HDIM), jnp.float32), -4.0, 4.0)
    scaled = raw_values * head_scale[None, :, None]
    return scaled.reshape(2, TOKEN_COUNT // 2, KVH * HDIM).astype(jnp.bfloat16)


def draw_log_decay(key, part):
    baseline_rate = jax.random.fold_in(key, 31)
    gradual_key, rate_key, quick_key, noise_key, spike_key, depth_key = jax.random.split(baseline_rate, 6)
    slow_share = 0.5
    slow_heads = jax.random.bernoulli(gradual_key, slow_share, (SHEADS,))
    slow_rate = jnp.exp(jax.random.uniform(rate_key, (SHEADS,), jnp.float32, jnp.log(0.1), jnp.log(0.6))) / TOKEN_COUNT
    fast_rate = jax.random.uniform(quick_key, (SHEADS,), jnp.float32, 1.0 / 50.0, 1.0 / 30.0)
    decay_speeds = jnp.where(slow_heads, slow_rate, fast_rate)
    random_noise = jnp.exp(jax.random.uniform(noise_key, (SHEADS, TOKEN_COUNT), jnp.float32, jnp.log(0.5), jnp.log(2.0)))
    spike_position = jax.random.randint(spike_key, (3,), 0, TOKEN_COUNT)
    spike_depth = jax.random.uniform(depth_key, (3,), jnp.float32, 0.22, 0.5)
    token_location = jnp.arange(TOKEN_COUNT)
    spike_events = jnp.sum(jnp.where(token_location[None, :] == spike_position[:, None], spike_depth[:, None], 0.0), axis=0)
    return -(decay_speeds[:, None] * random_noise + spike_events[None, :])


def block_levels(own_key, extent, cuts, least, largest):
    loudness = 1.0
    for dim, shards_of in cuts:
        heights = jax.random.uniform(jax.random.fold_in(jax.random.fold_in(own_key, 6), dim), (shards_of,), jnp.float32, least / len(cuts), largest / len(cuts))
        loudness = loudness * jnp.repeat(jnp.exp(heights), extent[dim] // shards_of).reshape((-1,) + (1,) * (len(extent) - 1 - dim))
    return loudness


def scatter_about(own_key, extent, spread, reach, cuts=(), kind=jnp.bfloat16):
    array = spread * jax.random.normal(own_key, extent, jnp.float32)
    if cuts:
        array = array * block_levels(own_key, extent, cuts, -0.22, 0.18)
    return jnp.clip(array, -reach, reach).astype(kind)


def setup_inputs(seed: int = 0) -> dict:
    key_list = jax.random.split(jax.random.key(seed), 10)
    query = draw_query(jax.random.fold_in(key_list[9], 71), 0)
    keys = draw_keys(jax.random.fold_in(key_list[9], 71), 0)
    values = draw_values(jax.random.fold_in(key_list[9], 71), 0)
    norm_gain = jnp.clip(1.0 + 0.15 * jax.random.normal(key_list[3], (HEADS * HDIM,), jnp.float32), 0.25, 1.75)
    in_b = scatter_about(key_list[4], (TOKEN_COUNT, STATE), 0.04, 0.25, ((0, 8),))
    out_c = scatter_about(key_list[5], (TOKEN_COUNT, STATE), 0.04, 0.25, ((0, 8),))
    step = jnp.clip(jnp.exp(math.log(1.0) - 1.609438 * jax.random.uniform(key_list[6], (SHEADS, TOKEN_COUNT), jnp.float32) ** block_levels(key_list[6], (SHEADS, TOKEN_COUNT), ((0, 4), (1, 8)), -0.2, 0.2)), 0.2, 1.0)
    log_decay = draw_log_decay(jax.random.fold_in(key_list[9], 71), 0)
    skip = jnp.clip(0.5 + 1.0 * jax.random.uniform(key_list[8], (SHEADS,), jnp.float32) ** block_levels(key_list[8], (SHEADS,), ((0, 4),), -0.2, 0.2), 0.5, 1.5)
    return {"query": query, "keys": keys, "values": values, "norm_gain": norm_gain, "in_b": in_b, "out_c": out_c, "step": step, "log_decay": log_decay, "skip": skip}


def attention_all(query, keys, values):
    group_size = HEADS // KVH
    queries = query.reshape(TOKEN_COUNT, KVH, group_size, HDIM)
    key_pad = jnp.concatenate([jnp.zeros((WIN, KVH, HDIM), jnp.bfloat16), keys.reshape(TOKEN_COUNT, KVH, HDIM)], 0)
    val_pad = jnp.concatenate([jnp.zeros((WIN, KVH, HDIM), jnp.bfloat16), values.reshape(TOKEN_COUNT, KVH, HDIM)], 0)
    score_scale = 1.0 / math.sqrt(HDIM)

    def attend_block(block_no):
        start = (block_no * BLK).astype(jnp.int32)
        query_rows = lax.dynamic_slice_in_dim(queries, start, BLK, 0).astype(jnp.float32)
        key_rows = lax.dynamic_slice_in_dim(key_pad, start, WIN + BLK, 0).astype(jnp.float32)
        val_rows = lax.dynamic_slice_in_dim(val_pad, start, WIN + BLK, 0).astype(jnp.float32)
        query_pos = start + jnp.arange(BLK, dtype=jnp.int32)
        key_pos = start - WIN + jnp.arange(WIN + BLK, dtype=jnp.int32)
        allowed = (key_pos[None, :] <= query_pos[:, None]) & (key_pos[None, :] > query_pos[:, None] - WIN) & (key_pos[None, :] >= 0)
        scores = jnp.einsum('qgjd,kgd->gjqk', query_rows, key_rows) * score_scale
        scores = jnp.where(allowed, scores, -jnp.inf)
        row_peak = lax.optimization_barrier(jnp.max(scores, axis=-1, keepdims=True))
        exp_terms = jnp.exp(scores - row_peak)
        row_total = lax.optimization_barrier(jnp.sum(exp_terms, axis=-1))
        weights = exp_terms.astype(jnp.bfloat16).astype(jnp.float32)
        result = jnp.einsum('gjqk,kgd->qgjd', weights, val_rows)
        result = result / jnp.transpose(row_total, (2, 0, 1))[..., None]
        return result.reshape(BLK, HEADS * HDIM).astype(jnp.bfloat16)
    blocks = lax.map(attend_block, jnp.arange(TOKEN_COUNT // BLK, dtype=jnp.int32))
    return blocks.reshape(TOKEN_COUNT, HEADS * HDIM)

def reference(query, keys, values, norm_gain, in_b, out_c, step, log_decay, skip):
    attended = attention_all(query, keys, values)
    widened = attended.astype(jnp.float32)
    meansq = lax.optimization_barrier(jnp.mean(widened * widened, axis=-1))
    normed = (widened * norm_gain[None, :] * lax.rsqrt(meansq + 1e-06)[:, None]).astype(jnp.bfloat16)
    span_count = TOKEN_COUNT // SPAN
    inputs = normed.astype(jnp.float32).reshape(span_count, SPAN, SHEADS, SDIM)
    in_rows = in_b.astype(jnp.float32).reshape(span_count, SPAN, STATE)
    out_rows = out_c.astype(jnp.float32).reshape(span_count, SPAN, STATE)
    step_rows = step.reshape(SHEADS, span_count, SPAN).transpose(1, 0, 2)
    decay_rows = log_decay.reshape(SHEADS, span_count, SPAN).transpose(1, 0, 2)
    causal = jnp.arange(SPAN)[:, None] >= jnp.arange(SPAN)[None, :]
    highest = lax.Precision.HIGHEST

    def advance(carried, pieces):
        x_rows, b_rows, c_rows, dt_rows, log_rows = pieces
        cum_log = jnp.cumsum(log_rows, axis=1)
        decay_mat = jnp.exp(jnp.where(causal[None], cum_log[:, :, None] - cum_log[:, None, :], -jnp.inf))
        cross_terms = jnp.dot(c_rows, b_rows.T, precision=highest)
        mixing = decay_mat * cross_terms[None] * dt_rows[:, None, :]
        mixing = mixing.astype(jnp.bfloat16).astype(jnp.float32)
        result = jnp.einsum('htu,uhe->the', mixing, x_rows, precision=highest)
        entry_term = jnp.einsum('tn,hen->the', c_rows, carried, precision=highest)
        result = result + entry_term * jnp.exp(cum_log).T[:, :, None]
        result = result + skip[None, :, None] * x_rows
        end_weights = jnp.exp(cum_log[:, -1:] - cum_log) * dt_rows
        weighted = end_weights.T[:, :, None] * x_rows
        carried = jnp.exp(cum_log[:, -1])[:, None, None] * carried + jnp.einsum('uhe,un->hen', weighted, b_rows, precision=highest)
        return (carried, result)
    initial = jnp.zeros((SHEADS, SDIM, STATE), jnp.float32)
    final_state, outputs = lax.scan(advance, initial, (inputs, in_rows, out_rows, step_rows, decay_rows))
    return outputs.reshape(TOKEN_COUNT, SHEADS * SDIM).astype(jnp.bfloat16)
```

```python
import functools
import math

import jax
import jax.numpy as jnp
from jax import lax
from jax.experimental import pallas as pl
from jax.experimental.pallas import tpu as pltpu
from jax.sharding import PartitionSpec as P

HDIM = 128
LANES = 128
F32 = jnp.float32
BF16 = jnp.bfloat16
MESH = pl.DeviceIdType.MESH


def remote(src, dst, send_sem, recv_sem, **where):
    return pltpu.make_async_remote_copy(
        src_ref=src,
        dst_ref=dst,
        send_sem=send_sem,
        recv_sem=recv_sem,
        device_id=where,
        device_id_type=MESH,
    )


def arrived(dst, sem):
    pltpu.make_async_copy(dst, dst, sem).wait()


def dot(a, b, dims, precision=None):
    return lax.dot_general(
        a, b, (dims, ((), ())), precision=precision, preferred_element_type=F32
    )


def kernel(
    n, nh,
    q_ref, k_ref, v_ref, gain_ref, b_ref, c_ref, step_ref, decay_ref, skip_ref,
    out_ref,
    q_buf, k_buf, v_buf, att, sumsq, mix, cum_buf, w_full, e_full, part,
    tot_buf, tot_own, ms_buf, ms_own, s_own, s_peer, t_chip, s_chips, p_own, p_peer,
    q_send, q_recv, kv_send, kv_recv, fwd_send,
    tot_send, tot_recv, ms_send, ms_recv, a_send, a_recv, b_send, b_recv, c_send, c_recv,
):
    me = lax.axis_index("seq")
    mz = lax.axis_index("head")
    core = lax.rem(me, 2)
    chip = me // 2
    chips = n // 2
    peer = me + 1 - 2 * core
    blk = q_ref.shape[1]
    feats = q_ref.shape[2]
    kv_local = k_ref.shape[2] // HDIM
    group = feats // HDIM // kv_local
    gcols = group * HDIM
    toks = 2 * blk
    heads = step_ref.shape[0]
    sdim = feats // heads
    tiles = feats // LANES
    half = feats // 2
    htiles = tiles // 2

    barrier = pltpu.get_barrier_semaphore()

    @pl.loop(1, n)
    def _(off):
        pl.semaphore_signal(
            barrier, inc=1, device_id={"seq": lax.rem(me + off, n)}, device_id_type=MESH
        )

    @pl.loop(1, nh)
    def _(off):
        pl.semaphore_signal(
            barrier, inc=1, device_id={"head": lax.rem(mz + off, nh)}, device_id_type=MESH
        )

    pl.semaphore_wait(barrier, n + nh - 2)

    def moves(g):
        found = []
        for s in range(2):
            home = (n // 2) * s + chip
            kcols = pl.ds(g * HDIM, HDIM)
            qcols = pl.ds(g * gcols, gcols)
            for t, (src, dst) in enumerate(((k_ref, k_buf), (v_ref, v_buf))):
                found.append((
                    src.at[s, :, kcols],
                    dst.at[pl.ds((2 + core) * blk, blk), kcols],
                    kv_send.at[g, s, 0, t], kv_recv.at[g, 2 + core, t], home, None,
                ))
                found.append((
                    src.at[s, :, kcols],
                    dst.at[pl.ds(core * blk, blk), kcols],
                    kv_send.at[g, s, 1, t], kv_recv.at[g, core, t], home + 1,
                    (lax.rem(home, 2) == 1) & (home + 1 < n),
                ))
            found.append((
                q_ref.at[s, :, qcols],
                q_buf.at[pl.ds(core * blk, blk), qcols],
                q_send.at[g, s], q_recv.at[g, core], home, None,
            ))
        return found

    def away(dest, cond):
        other = dest != me
        return other if cond is None else other & cond

    for g in range(kv_local):
        for src, dst, ssem, rsem, dest, cond in moves(g):

            @pl.when(away(dest, cond))
            def _():
                remote(src, dst, ssem, rsem, seq=dest).start()

            here = dest == me
            here = here if cond is None else here & cond

            @pl.when(here)
            def _():
                pltpu.make_async_copy(src, dst, rsem).start()

    @pl.when(me == 0)
    def _():
        k_buf[0:toks] = jnp.zeros_like(k_buf[0:toks])
        v_buf[0:toks] = jnp.zeros_like(v_buf[0:toks])

    t_ids = lax.broadcasted_iota(jnp.int32, (toks, toks), 0)
    u_ids = lax.broadcasted_iota(jnp.int32, (toks, toks), 1)
    upper = (t_ids <= u_ids).astype(F32)
    cum = dot(decay_ref[...], upper, ((1,), (0,)), lax.Precision.HIGHEST)
    cum_buf[...] = cum
    pick = (
        lax.broadcasted_iota(jnp.int32, (heads, feats), 1) // sdim
        == lax.broadcasted_iota(jnp.int32, (heads, feats), 0)
    ).astype(F32)
    total = jnp.sum(decay_ref[...], axis=1, keepdims=True)
    tot_row = jnp.sum(total * pick, axis=0, keepdims=True)
    for p in range(tiles):
        tot_own[p : p + 1, :] = tot_row[:, p * LANES : (p + 1) * LANES]

    def tot_copy(dest, source):
        return remote(
            tot_own, tot_buf.at[source], tot_send.at[dest], tot_recv.at[source], seq=dest
        )

    @pl.loop(1, n)
    def _(off):
        tot_copy(lax.rem(me + off, n), me).start()

    tot_buf[me] = tot_own[...]

    def expand(rows):
        high = rows.astype(BF16)
        low = (rows - high.astype(F32)).astype(BF16)
        both = jnp.concatenate([high, low], 0)
        pick2 = jnp.concatenate([pick, pick], 0).astype(BF16)
        return dot(both, pick2, ((0,), (0,)))

    w_full[...] = expand(jnp.exp(cum[:, toks - 1 : toks] - cum) * step_ref[...])
    e_full[...] = expand(jnp.exp(cum))
    cross = dot(c_ref[...], b_ref[...], ((1,), (1,)))
    part[:, 0:toks] = jnp.where(t_ids >= u_ids, cross, 0.0)

    @pl.loop(0, heads)
    def _(h):
        row = cum_buf[pl.ds(h, 1), :]
        col = jnp.transpose(jnp.broadcast_to(row, (LANES, toks)))
        srow = step_ref[pl.ds(h, 1), :]
        for lo in range(0, toks, LANES):
            cols = slice(lo, lo + LANES)
            diff = jnp.minimum(col - row[:, cols], 0.0)
            mix[h, :, cols] = (jnp.exp(diff) * part[:, cols] * srow[:, cols]).astype(BF16)

    factor = math.log2(math.e) / math.sqrt(HDIM)
    r_ids = lax.broadcasted_iota(jnp.int32, (blk, blk), 0)
    c_ids = lax.broadcasted_iota(jnp.int32, (blk, blk), 1)
    sumsq[...] = jnp.zeros_like(sumsq)
    for g in range(kv_local):
        kcols = slice(g * HDIM, (g + 1) * HDIM)
        for slot in (2, 3):
            for t, buf in enumerate((k_buf, v_buf)):
                arrived(
                    buf.at[pl.ds(slot * blk, blk), pl.ds(g * HDIM, HDIM)],
                    kv_recv.at[g, slot, t],
                )

        @pl.when(core == 0)
        def _():
            for slot in (2, 3):
                for t, buf in enumerate((k_buf, v_buf)):
                    remote(
                        buf.at[pl.ds(slot * blk, blk), pl.ds(g * HDIM, HDIM)],
                        buf.at[pl.ds((slot - 2) * blk, blk), pl.ds(g * HDIM, HDIM)],
                        fwd_send.at[g, slot - 2, t], kv_recv.at[g, slot - 2, t], seq=peer,
                    ).start()

        @pl.when(me > 0)
        def _():
            for slot in (0, 1):
                for t, buf in enumerate((k_buf, v_buf)):
                    arrived(
                        buf.at[pl.ds(slot * blk, blk), pl.ds(g * HDIM, HDIM)],
                        kv_recv.at[g, slot, t],
                    )

        for slot in (0, 1):
            arrived(
                q_buf.at[pl.ds(slot * blk, blk), pl.ds(g * gcols, gcols)], q_recv.at[g, slot]
            )

        @pl.loop(0, group)
        def _(j):
            hcols = pl.ds(pl.multiple_of(g * gcols + j * HDIM, HDIM), HDIM)
            for slot in (0, 1):
                rows = slice(slot * blk, (slot + 1) * blk)
                keys = slice(slot * blk, (slot + 3) * blk)
                score = dot(q_buf[rows, hcols], k_buf[keys, kcols], ((1,), (1,)))
                far = (c_ids > r_ids) & (me > 0)
                mid = None if slot else jnp.broadcast_to(me > 0, (blk, blk))
                s0 = jnp.where(far, score[:, 0:blk], -jnp.inf)
                s1 = score[:, blk : 2 * blk]
                if slot == 0:
                    s1 = jnp.where(mid, s1, -jnp.inf)
                s2 = jnp.where(c_ids <= r_ids, score[:, 2 * blk :], -jnp.inf)
                peak = jnp.max(jnp.maximum(jnp.maximum(s0, s1), s2), axis=1, keepdims=True)
                e0 = jnp.exp2((s0 - peak) * factor)
                e1 = jnp.exp2((s1 - peak) * factor)
                e2 = jnp.exp2((s2 - peak) * factor)
                weight = jnp.concatenate([e0, e1, e2], 1).astype(BF16)
                whole = jnp.sum(e0 + e1 + e2, axis=1, keepdims=True)
                result = dot(weight, v_buf[keys, kcols], ((1,), (0,))) / whole
                result = result.astype(BF16)
                att[rows, hcols] = result
                wide = result.astype(F32)
                sumsq[rows, :] += wide * wide

    ms_row = jnp.sum(jnp.transpose(sumsq[...]), axis=0, keepdims=True)
    ms_own[...] = jnp.broadcast_to(ms_row, ms_own.shape)

    def ms_copy(dest, source):
        return remote(
            ms_own, ms_buf.at[source], ms_send.at[dest], ms_recv.at[source], head=dest
        )

    @pl.loop(1, nh)
    def _(off):
        ms_copy(lax.rem(mz + off, nh), mz).start()

    ms_buf[mz] = ms_own[...]

    @pl.loop(1, nh)
    def _(off):
        arrived(ms_buf.at[lax.rem(mz + off, nh)], ms_recv.at[lax.rem(mz + off, nh)])

    meansq = jnp.sum(ms_buf[...], axis=0)[0:1, :] * (1.0 / (feats * nh))
    scale = jnp.transpose(jnp.broadcast_to(lax.rsqrt(meansq + 1e-06), (LANES, toks)))

    b_turned = jnp.transpose(b_ref[...].astype(F32)).astype(BF16)
    for p in range(tiles):
        cols = slice(p * LANES, (p + 1) * LANES)
        normed = (att[:, cols].astype(F32) * gain_ref[:, cols] * scale).astype(BF16)
        att[:, cols] = normed
        scaled = (normed.astype(F32) * w_full[:, cols]).astype(BF16)
        into = slice((p % htiles) * LANES, (p % htiles + 1) * LANES)
        s_own[p // htiles, :, into] = dot(b_turned, scaled, ((1,), (0,))).astype(BF16)

    a_copy = remote(s_own, s_peer, a_send, a_recv, seq=peer)
    a_copy.start()

    @pl.loop(1, n)
    def _(off):
        arrived(tot_buf.at[lax.rem(me + off, n)], tot_recv.at[lax.rem(me + off, n)])

    def row_of(device, side):
        return jnp.concatenate(
            [tot_buf[device, pl.ds(side * htiles + q, 1), :] for q in range(htiles)], 1
        )

    even = core == 0
    one = jnp.ones((1, half), F32)
    mine_scale = jnp.where(even, jnp.exp(row_of(peer, core)), one)
    peer_scale = jnp.where(even, one, jnp.exp(row_of(me, core)))
    a_copy.wait_recv()
    t_chip[...] = (
        mine_scale * s_own[core].astype(F32) + peer_scale * s_peer[core].astype(F32)
    ).astype(BF16)

    def b_copy(dest, source):
        return remote(
            t_chip, s_chips.at[source], b_send.at[dest], b_recv.at[source],
            seq=2 * dest + core,
        )

    @pl.loop(chip + 1, chips)
    def _(dest):
        b_copy(dest, chip).start()

    left = lax.broadcasted_iota(jnp.int32, (toks, LANES), 1) < sdim
    skip_row = jnp.sum(skip_ref[...] * pick, axis=0, keepdims=True)
    for p in range(tiles):
        cols = slice(p * LANES, (p + 1) * LANES)
        x = att[:, cols]
        zero = jnp.zeros_like(x)
        y = dot(mix[2 * p], jnp.where(left, x, zero), ((1,), (0,)))
        y += dot(mix[2 * p + 1], jnp.where(left, zero, x), ((1,), (0,)))
        part[:, cols] = y + skip_row[:, cols] * x.astype(F32)

    w_full[0 : s_own.shape[1], 0:half] = jnp.zeros((s_own.shape[1], half), F32)
    state = w_full.at[0 : s_own.shape[1], 0:half]

    @pl.loop(0, chip)
    def _(source):
        arrived(s_chips.at[source], b_recv.at[source])
        decay = jnp.exp(row_of(2 * source, core) + row_of(2 * source + 1, core))
        state[...] = decay * state[...] + s_chips[source].astype(F32)

    p_own[...] = state[...].astype(BF16)
    c_copy = remote(p_own, p_peer, c_send, c_recv, seq=peer)
    c_copy.start()

    def finish(side, entered):
        lanes = slice(side * half, (side + 1) * half)
        keep = jnp.where(even, one, jnp.exp(row_of(peer, side)))
        add = jnp.where(even, jnp.zeros_like(one), one)
        entering = keep * entered.astype(F32) + add * s_peer[side].astype(F32)
        term = dot(c_ref[...], entering.astype(BF16), ((1,), (0,)))
        out_ref[:, lanes] = (part[:, lanes] + term * e_full[:, lanes]).astype(BF16)

    c_copy.wait_recv()
    for side in range(2):
        finish(side, jnp.where(core == side, p_own[...], p_peer[...]))

    for g in range(kv_local):
        for src, dst, ssem, rsem, dest, cond in moves(g):

            @pl.when(away(dest, cond))
            def _():
                remote(src, dst, ssem, rsem, seq=dest).wait_send()

        @pl.when(core == 0)
        def _():
            for slot in (2, 3):
                for t, buf in enumerate((k_buf, v_buf)):
                    remote(
                        buf.at[pl.ds(slot * blk, blk), pl.ds(g * HDIM, HDIM)],
                        buf.at[pl.ds((slot - 2) * blk, blk), pl.ds(g * HDIM, HDIM)],
                        fwd_send.at[g, slot - 2, t], kv_recv.at[g, slot - 2, t], seq=peer,
                    ).wait_send()

    @pl.loop(1, n)
    def _(off):
        tot_copy(lax.rem(me + off, n), me).wait_send()

    @pl.loop(1, nh)
    def _(off):
        ms_copy(lax.rem(mz + off, nh), mz).wait_send()

    @pl.loop(chip + 1, chips)
    def _(dest):
        b_copy(dest, chip).wait_send()

    a_copy.wait_send()
    c_copy.wait_send()


def body(query, keys, values, norm_gain, in_b, out_c, step, log_decay, skip):
    n = lax.axis_size("seq")
    nh = lax.axis_size("head")
    blk, feats = query.shape[1], query.shape[2]
    kvcols = keys.shape[2]
    kv_local = kvcols // HDIM
    toks = 2 * blk
    heads = step.shape[0]
    nstate = in_b.shape[1]
    tiles = feats // LANES
    half = feats // 2
    chips = n // 2
    dma = pltpu.SemaphoreType.DMA
    vmem = pl.BlockSpec(memory_space=pltpu.VMEM)
    return pl.pallas_call(
        functools.partial(kernel, n, nh),
        out_shape=jax.ShapeDtypeStruct((toks, feats), BF16),
        in_specs=[vmem] * 9,
        out_specs=vmem,
        scratch_shapes=[
            pltpu.VMEM((toks, feats), BF16),
            pltpu.VMEM((2 * toks, kvcols), BF16),
            pltpu.VMEM((2 * toks, kvcols), BF16),
            pltpu.VMEM((toks, feats), BF16),
            pltpu.VMEM((toks, LANES), F32),
            pltpu.VMEM((heads, toks, toks), BF16),
            pltpu.VMEM((heads, toks), F32),
            pltpu.VMEM((toks, feats), F32),
            pltpu.VMEM((toks, feats), F32),
            pltpu.VMEM((toks, feats), F32),
            pltpu.VMEM((n, tiles, LANES), F32),
            pltpu.VMEM((tiles, LANES), F32),
            pltpu.VMEM((nh, 8, toks), F32),
            pltpu.VMEM((8, toks), F32),
            pltpu.VMEM((2, nstate, half), BF16),
            pltpu.VMEM((2, nstate, half), BF16),
            pltpu.VMEM((nstate, half), BF16),
            pltpu.VMEM((chips, nstate, half), BF16),
            pltpu.VMEM((nstate, half), BF16),
            pltpu.VMEM((nstate, half), BF16),
            dma((kv_local, 2)), dma((kv_local, 2)),
            dma((kv_local, 2, 2, 2)), dma((kv_local, 4, 2)), dma((kv_local, 2, 2)),
            dma((n,)), dma((n,)), dma((nh,)), dma((nh,)),
            dma, dma, dma((chips,)), dma((chips,)), dma, dma,
        ],
        compiler_params=pltpu.CompilerParams(
            collective_id=0, has_side_effects=True, vmem_limit_bytes=60 * 2**20
        ),
    )(
        query, keys, values, norm_gain.reshape(1, feats), in_b, out_c, step, log_decay,
        skip.reshape(heads, 1),
    )


def solution(mesh):
    placed = (
        P(None, "seq", "head"),
        P(None, "seq", "head"),
        P(None, "seq", "head"),
        P("head"),
        P("seq", None),
        P("seq", None),
        P("head", "seq"),
        P("head", "seq"),
        P("head"),
    )
    return jax.shard_map(
        body, mesh=mesh, in_specs=placed, out_specs=P("seq", "head"), check_vma=False
    )
```

```python
import functools
import math

import jax
import jax.numpy as jnp
from jax import lax
from jax.experimental import pallas as pl
from jax.experimental.pallas import tpu as pltpu
from jax.sharding import PartitionSpec as P

HDIM = 128
LANES = 128
F32 = jnp.float32
BF16 = jnp.bfloat16
MESH = pl.DeviceIdType.MESH


def remote(src, dst, send_sem, recv_sem, **where):
    return pltpu.make_async_remote_copy(
        src_ref=src,
        dst_ref=dst,
        send_sem=send_sem,
        recv_sem=recv_sem,
        device_id=where,
        device_id_type=MESH,
    )


def arrived(dst, sem):
    pltpu.make_async_copy(dst, dst, sem).wait()


def dot(a, b, dims, precision=None):
    return lax.dot_general(
        a, b, (dims, ((), ())), precision=precision, preferred_element_type=F32
    )


def kernel(
    n, nh,
    q_ref, k_ref, v_ref, gain_ref, b_ref, c_ref, step_ref, decay_ref, skip_ref,
    out_ref,
    q_buf, k_buf, v_buf, att, sumsq, mix, cum_buf, w_full, e_full, part,
    tot_buf, tot_own, ms_buf, ms_own, s_own, s_peer, t_chip, s_chips, p_own, p_peer,
    q_send, q_recv, kv_send, kv_recv, fwd_send,
    tot_send, tot_recv, ms_send, ms_recv, a_send, a_recv, b_send, b_recv, c_send, c_recv,
    rel_k, rel_v, rel_q, rel_send, rel_recv,
):
    me = lax.axis_index("seq")
    mz = lax.axis_index("head")
    core = lax.rem(me, 2)
    chip = me // 2
    chips = n // 2
    peer = me + 1 - 2 * core
    blk = q_ref.shape[1]
    feats = q_ref.shape[2]
    kv_local = k_ref.shape[2] // HDIM
    group = feats // HDIM // kv_local
    gcols = group * HDIM
    toks = 2 * blk
    heads = step_ref.shape[0]
    sdim = feats // heads
    tiles = feats // LANES
    half = feats // 2
    htiles = tiles // 2

    barrier = pltpu.get_barrier_semaphore()

    @pl.loop(1, n)
    def _(off):
        pl.semaphore_signal(
            barrier, inc=1, device_id={"seq": lax.rem(me + off, n)}, device_id_type=MESH
        )

    @pl.loop(1, nh)
    def _(off):
        pl.semaphore_signal(
            barrier, inc=1, device_id={"head": lax.rem(mz + off, nh)}, device_id_type=MESH
        )

    pl.semaphore_wait(barrier, n + nh - 2)

    quarter = n // 4

    def crosses(s):
        goal = quarter * s + chip // 2
        via = 2 * (2 * (goal // 2) + lax.rem(chip, 2)) + core
        return (lax.rem(goal, 2) != lax.rem(chip, 2)) & (goal // 2 != chip // 2), via

    goal_chip = 2 * (chip // 2) + 1 - lax.rem(chip, 2)
    relaying = lax.rem(goal_chip, quarter) != chip // 2
    goal = 2 * goal_chip + lax.rem(chip, 2)

    def relay(g):
        kcols = pl.ds(g * HDIM, HDIM)
        qcols = pl.ds(g * gcols, gcols)
        rows = pl.ds(core * blk, blk)
        krows = pl.ds((2 + core) * blk, blk)
        return (
            (rel_k.at[:, kcols], k_buf.at[krows, kcols], 0, kv_recv.at[g, 2 + core, 0]),
            (rel_v.at[:, kcols], v_buf.at[krows, kcols], 1, kv_recv.at[g, 2 + core, 1]),
            (rel_q.at[:, qcols], q_buf.at[rows, qcols], 2, q_recv.at[g, core]),
        )

    def pass_on(g):
        @pl.when(relaying)
        def _():
            for held, dst, t, rsem in relay(g):
                arrived(held, rel_recv.at[g, t])
                remote(held, dst, rel_send.at[g, t], rsem, seq=goal).start()

    def moves(g):
        found = []
        for s in range(2):
            home = (n // 2) * s + chip
            diag, via = crosses(s)
            straight = jnp.logical_not(diag)
            kcols = pl.ds(g * HDIM, HDIM)
            qcols = pl.ds(g * gcols, gcols)
            for t, (src, dst) in enumerate(((k_ref, k_buf), (v_ref, v_buf))):
                found.append((
                    src.at[s, :, kcols],
                    dst.at[pl.ds((2 + core) * blk, blk), kcols],
                    kv_send.at[g, s, 0, t], kv_recv.at[g, 2 + core, t], home, straight,
                ))
                found.append((
                    src.at[s, :, kcols], (rel_k, rel_v)[t].at[:, kcols],
                    kv_send.at[g, s, 0, t], rel_recv.at[g, t], via, diag,
                ))
                found.append((
                    src.at[s, :, kcols],
                    dst.at[pl.ds(core * blk, blk), kcols],
                    kv_send.at[g, s, 1, t], kv_recv.at[g, core, t], home + 1,
                    (lax.rem(home, 2) == 1) & (home + 1 < n),
                ))
            found.append((
                q_ref.at[s, :, qcols],
                q_buf.at[pl.ds(core * blk, blk), qcols],
                q_send.at[g, s], q_recv.at[g, core], home, straight,
            ))
            found.append((
                q_ref.at[s, :, qcols], rel_q.at[:, qcols],
                q_send.at[g, s], rel_recv.at[g, 2], via, diag,
            ))
        return found

    def away(dest, cond):
        other = dest != me
        return other if cond is None else other & cond

    for g in range(kv_local):
        for src, dst, ssem, rsem, dest, cond in moves(g):

            @pl.when(away(dest, cond))
            def _():
                remote(src, dst, ssem, rsem, seq=dest).start()

            here = dest == me
            here = here if cond is None else here & cond

            @pl.when(here)
            def _():
                pltpu.make_async_copy(src, dst, rsem).start()

    @pl.when(me == 0)
    def _():
        k_buf[0:toks] = jnp.zeros_like(k_buf[0:toks])
        v_buf[0:toks] = jnp.zeros_like(v_buf[0:toks])

    t_ids = lax.broadcasted_iota(jnp.int32, (toks, toks), 0)
    u_ids = lax.broadcasted_iota(jnp.int32, (toks, toks), 1)
    upper = (t_ids <= u_ids).astype(F32)
    cum = dot(decay_ref[...], upper, ((1,), (0,)), lax.Precision.HIGHEST)
    cum_buf[...] = cum
    pick = (
        lax.broadcasted_iota(jnp.int32, (heads, feats), 1) // sdim
        == lax.broadcasted_iota(jnp.int32, (heads, feats), 0)
    ).astype(F32)
    total = jnp.sum(decay_ref[...], axis=1, keepdims=True)
    tot_row = jnp.sum(total * pick, axis=0, keepdims=True)
    for p in range(tiles):
        tot_own[p : p + 1, :] = tot_row[:, p * LANES : (p + 1) * LANES]

    def tot_copy(dest, source):
        return remote(
            tot_own, tot_buf.at[source], tot_send.at[dest], tot_recv.at[source], seq=dest
        )

    @pl.loop(1, n)
    def _(off):
        tot_copy(lax.rem(me + off, n), me).start()

    tot_buf[me] = tot_own[...]

    def expand(rows):
        high = rows.astype(BF16)
        low = (rows - high.astype(F32)).astype(BF16)
        both = jnp.concatenate([high, low], 0)
        pick2 = jnp.concatenate([pick, pick], 0).astype(BF16)
        return dot(both, pick2, ((0,), (0,)))

    w_full[...] = expand(jnp.exp(cum[:, toks - 1 : toks] - cum) * step_ref[...])
    e_full[...] = expand(jnp.exp(cum))
    cross = dot(c_ref[...], b_ref[...], ((1,), (1,)))
    part[:, 0:toks] = jnp.where(t_ids >= u_ids, cross, 0.0)

    def mix_head(h):
        row = cum_buf[pl.ds(h, 1), :]
        col = jnp.transpose(jnp.broadcast_to(row, (LANES, toks)))
        srow = step_ref[pl.ds(h, 1), :]
        for lo in range(0, toks, LANES):
            cols = slice(lo, lo + LANES)
            diff = jnp.minimum(col - row[:, cols], 0.0)
            mix[h, :, cols] = (jnp.exp(diff) * part[:, cols] * srow[:, cols]).astype(BF16)

    per = heads // kv_local
    for g in range(kv_local):
        pl.loop(g * per, (g + 1) * per)(mix_head)
        pass_on(g)

    factor = math.log2(math.e) / math.sqrt(HDIM)
    r_ids = lax.broadcasted_iota(jnp.int32, (blk, blk), 0)
    c_ids = lax.broadcasted_iota(jnp.int32, (blk, blk), 1)
    sumsq[...] = jnp.zeros_like(sumsq)
    for g in range(kv_local):
        kcols = slice(g * HDIM, (g + 1) * HDIM)
        for slot in (2, 3):
            for t, buf in enumerate((k_buf, v_buf)):
                arrived(
                    buf.at[pl.ds(slot * blk, blk), pl.ds(g * HDIM, HDIM)],
                    kv_recv.at[g, slot, t],
                )

        @pl.when(core == 0)
        def _():
            for slot in (2, 3):
                for t, buf in enumerate((k_buf, v_buf)):
                    remote(
                        buf.at[pl.ds(slot * blk, blk), pl.ds(g * HDIM, HDIM)],
                        buf.at[pl.ds((slot - 2) * blk, blk), pl.ds(g * HDIM, HDIM)],
                        fwd_send.at[g, slot - 2, t], kv_recv.at[g, slot - 2, t], seq=peer,
                    ).start()

        @pl.when(me > 0)
        def _():
            for slot in (0, 1):
                for t, buf in enumerate((k_buf, v_buf)):
                    arrived(
                        buf.at[pl.ds(slot * blk, blk), pl.ds(g * HDIM, HDIM)],
                        kv_recv.at[g, slot, t],
                    )

        for slot in (0, 1):
            arrived(
                q_buf.at[pl.ds(slot * blk, blk), pl.ds(g * gcols, gcols)], q_recv.at[g, slot]
            )

        @pl.loop(0, group)
        def _(j):
            hcols = pl.ds(pl.multiple_of(g * gcols + j * HDIM, HDIM), HDIM)
            for slot in (0, 1):
                rows = slice(slot * blk, (slot + 1) * blk)
                keys = slice(slot * blk, (slot + 3) * blk)
                score = dot(q_buf[rows, hcols], k_buf[keys, kcols], ((1,), (1,)))
                far = (c_ids > r_ids) & (me > 0)
                mid = None if slot else jnp.broadcast_to(me > 0, (blk, blk))
                s0 = jnp.where(far, score[:, 0:blk], -jnp.inf)
                s1 = score[:, blk : 2 * blk]
                if slot == 0:
                    s1 = jnp.where(mid, s1, -jnp.inf)
                s2 = jnp.where(c_ids <= r_ids, score[:, 2 * blk :], -jnp.inf)
                peak = jnp.max(jnp.maximum(jnp.maximum(s0, s1), s2), axis=1, keepdims=True)
                e0 = jnp.exp2((s0 - peak) * factor)
                e1 = jnp.exp2((s1 - peak) * factor)
                e2 = jnp.exp2((s2 - peak) * factor)
                weight = jnp.concatenate([e0, e1, e2], 1).astype(BF16)
                whole = jnp.sum(e0 + e1 + e2, axis=1, keepdims=True)
                result = dot(weight, v_buf[keys, kcols], ((1,), (0,))) / whole
                result = result.astype(BF16)
                att[rows, hcols] = result
                wide = result.astype(F32)
                sumsq[rows, :] += wide * wide

    ms_row = jnp.sum(jnp.transpose(sumsq[...]), axis=0, keepdims=True)
    ms_own[...] = jnp.broadcast_to(ms_row, ms_own.shape)

    def ms_copy(dest, source):
        return remote(
            ms_own, ms_buf.at[source], ms_send.at[dest], ms_recv.at[source], head=dest
        )

    @pl.loop(1, nh)
    def _(off):
        ms_copy(lax.rem(mz + off, nh), mz).start()

    ms_buf[mz] = ms_own[...]

    @pl.loop(1, nh)
    def _(off):
        arrived(ms_buf.at[lax.rem(mz + off, nh)], ms_recv.at[lax.rem(mz + off, nh)])

    meansq = jnp.sum(ms_buf[...], axis=0)[0:1, :] * (1.0 / (feats * nh))
    scale = jnp.transpose(jnp.broadcast_to(lax.rsqrt(meansq + 1e-06), (LANES, toks)))

    b_turned = jnp.transpose(b_ref[...].astype(F32)).astype(BF16)
    for p in range(tiles):
        cols = slice(p * LANES, (p + 1) * LANES)
        normed = (att[:, cols].astype(F32) * gain_ref[:, cols] * scale).astype(BF16)
        att[:, cols] = normed
        scaled = (normed.astype(F32) * w_full[:, cols]).astype(BF16)
        into = slice((p % htiles) * LANES, (p % htiles + 1) * LANES)
        s_own[p // htiles, :, into] = dot(b_turned, scaled, ((1,), (0,))).astype(BF16)

    a_copy = remote(s_own, s_peer, a_send, a_recv, seq=peer)
    a_copy.start()

    @pl.loop(1, n)
    def _(off):
        arrived(tot_buf.at[lax.rem(me + off, n)], tot_recv.at[lax.rem(me + off, n)])

    def row_of(device, side):
        return jnp.concatenate(
            [tot_buf[device, pl.ds(side * htiles + q, 1), :] for q in range(htiles)], 1
        )

    even = core == 0
    one = jnp.ones((1, half), F32)
    mine_scale = jnp.where(even, jnp.exp(row_of(peer, core)), one)
    peer_scale = jnp.where(even, one, jnp.exp(row_of(me, core)))
    a_copy.wait_recv()
    t_chip[...] = (
        mine_scale * s_own[core].astype(F32) + peer_scale * s_peer[core].astype(F32)
    ).astype(BF16)

    def b_copy(dest, source):
        return remote(
            t_chip, s_chips.at[source], b_send.at[dest], b_recv.at[source],
            seq=2 * dest + core,
        )

    @pl.loop(chip + 1, chips)
    def _(dest):
        b_copy(dest, chip).start()

    left = lax.broadcasted_iota(jnp.int32, (toks, LANES), 1) < sdim
    skip_row = dot(skip_ref[...], pick, ((1,), (0,)), lax.Precision.HIGHEST)
    for p in range(tiles):
        cols = slice(p * LANES, (p + 1) * LANES)
        x = att[:, cols]
        zero = jnp.zeros_like(x)
        y = dot(mix[2 * p], jnp.where(left, x, zero), ((1,), (0,)))
        y += dot(mix[2 * p + 1], jnp.where(left, zero, x), ((1,), (0,)))
        part[:, cols] = y + skip_row[:, cols] * x.astype(F32)

    w_full[0 : s_own.shape[1], 0:half] = jnp.zeros((s_own.shape[1], half), F32)
    state = w_full.at[0 : s_own.shape[1], 0:half]

    @pl.loop(0, chip)
    def _(source):
        arrived(s_chips.at[source], b_recv.at[source])
        decay = jnp.exp(row_of(2 * source, core) + row_of(2 * source + 1, core))
        state[...] = decay * state[...] + s_chips[source].astype(F32)

    p_own[...] = state[...].astype(BF16)
    c_copy = remote(p_own, p_peer, c_send, c_recv, seq=peer)
    c_copy.start()

    def finish(side, entered):
        lanes = slice(side * half, (side + 1) * half)
        keep = jnp.where(even, one, jnp.exp(row_of(peer, side)))
        add = jnp.where(even, jnp.zeros_like(one), one)
        entering = keep * entered.astype(F32) + add * s_peer[side].astype(F32)
        term = dot(c_ref[...], entering.astype(BF16), ((1,), (0,)))
        out_ref[:, lanes] = (part[:, lanes] + term * e_full[:, lanes]).astype(BF16)

    c_copy.wait_recv()
    for side in range(2):
        finish(side, jnp.where(core == side, p_own[...], p_peer[...]))

    for g in range(kv_local):
        for src, dst, ssem, rsem, dest, cond in moves(g):

            @pl.when(away(dest, cond))
            def _():
                remote(src, dst, ssem, rsem, seq=dest).wait_send()

        @pl.when(relaying)
        def _():
            for held, dst, t, rsem in relay(g):
                remote(held, dst, rel_send.at[g, t], rsem, seq=goal).wait_send()

        @pl.when(core == 0)
        def _():
            for slot in (2, 3):
                for t, buf in enumerate((k_buf, v_buf)):
                    remote(
                        buf.at[pl.ds(slot * blk, blk), pl.ds(g * HDIM, HDIM)],
                        buf.at[pl.ds((slot - 2) * blk, blk), pl.ds(g * HDIM, HDIM)],
                        fwd_send.at[g, slot - 2, t], kv_recv.at[g, slot - 2, t], seq=peer,
                    ).wait_send()

    @pl.loop(1, n)
    def _(off):
        tot_copy(lax.rem(me + off, n), me).wait_send()

    @pl.loop(1, nh)
    def _(off):
        ms_copy(lax.rem(mz + off, nh), mz).wait_send()

    @pl.loop(chip + 1, chips)
    def _(dest):
        b_copy(dest, chip).wait_send()

    a_copy.wait_send()
    c_copy.wait_send()


def body(query, keys, values, norm_gain, in_b, out_c, step, log_decay, skip):
    n = lax.axis_size("seq")
    nh = lax.axis_size("head")
    blk, feats = query.shape[1], query.shape[2]
    kvcols = keys.shape[2]
    kv_local = kvcols // HDIM
    toks = 2 * blk
    heads = step.shape[0]
    nstate = in_b.shape[1]
    tiles = feats // LANES
    half = feats // 2
    chips = n // 2
    dma = pltpu.SemaphoreType.DMA
    vmem = pl.BlockSpec(memory_space=pltpu.VMEM)
    return pl.pallas_call(
        functools.partial(kernel, n, nh),
        out_shape=jax.ShapeDtypeStruct((toks, feats), BF16),
        in_specs=[vmem] * 9,
        out_specs=vmem,
        scratch_shapes=[
            pltpu.VMEM((toks, feats), BF16),
            pltpu.VMEM((2 * toks, kvcols), BF16),
            pltpu.VMEM((2 * toks, kvcols), BF16),
            pltpu.VMEM((toks, feats), BF16),
            pltpu.VMEM((toks, LANES), F32),
            pltpu.VMEM((heads, toks, toks), BF16),
            pltpu.VMEM((heads, toks), F32),
            pltpu.VMEM((toks, feats), F32),
            pltpu.VMEM((toks, feats), F32),
            pltpu.VMEM((toks, feats), F32),
            pltpu.VMEM((n, tiles, LANES), F32),
            pltpu.VMEM((tiles, LANES), F32),
            pltpu.VMEM((nh, 8, toks), F32),
            pltpu.VMEM((8, toks), F32),
            pltpu.VMEM((2, nstate, half), BF16),
            pltpu.VMEM((2, nstate, half), BF16),
            pltpu.VMEM((nstate, half), BF16),
            pltpu.VMEM((chips, nstate, half), BF16),
            pltpu.VMEM((nstate, half), BF16),
            pltpu.VMEM((nstate, half), BF16),
            dma((kv_local, 2)), dma((kv_local, 2)),
            dma((kv_local, 2, 2, 2)), dma((kv_local, 4, 2)), dma((kv_local, 2, 2)),
            dma((n,)), dma((n,)), dma((nh,)), dma((nh,)),
            dma, dma, dma((chips,)), dma((chips,)), dma, dma,
            pltpu.VMEM((blk, kvcols), BF16),
            pltpu.VMEM((blk, kvcols), BF16),
            pltpu.VMEM((blk, feats), BF16),
            dma((kv_local, 3)), dma((kv_local, 3)),
        ],
        compiler_params=pltpu.CompilerParams(
            collective_id=0, has_side_effects=True, vmem_limit_bytes=60 * 2**20
        ),
    )(
        query, keys, values, norm_gain.reshape(1, feats), in_b, out_c, step, log_decay,
        skip.reshape(1, heads),
    )


def solution(mesh):
    placed = (
        P(None, "seq", "head"),
        P(None, "seq", "head"),
        P(None, "seq", "head"),
        P("head"),
        P("seq", None),
        P("seq", None),
        P("head", "seq"),
        P("head", "seq"),
        P("head"),
    )
    return jax.shard_map(
        body, mesh=mesh, in_specs=placed, out_specs=P("seq", "head"), check_vma=False
    )
```

```python
import functools
import math

import jax
import jax.numpy as jnp
from jax import lax
from jax.experimental import pallas as pl
from jax.experimental.pallas import tpu as pltpu
from jax.sharding import PartitionSpec as P

HDIM = 128
LANES = 128
F32 = jnp.float32
BF16 = jnp.bfloat16
MESH = pl.DeviceIdType.MESH


def remote(src, dst, send_sem, recv_sem, **where):
    return pltpu.make_async_remote_copy(
        src_ref=src,
        dst_ref=dst,
        send_sem=send_sem,
        recv_sem=recv_sem,
        device_id=where,
        device_id_type=MESH,
    )


def arrived(dst, sem):
    pltpu.make_async_copy(dst, dst, sem).wait()


def dot(a, b, dims, precision=None):
    return lax.dot_general(
        a, b, (dims, ((), ())), precision=precision, preferred_element_type=F32
    )


def kernel(
    n, nh,
    q_ref, k_ref, v_ref, gain_ref, b_ref, c_ref, step_ref, decay_ref, skip_ref,
    out_ref,
    q_buf, k_buf, v_buf, att, sumsq, mix, cum_buf, w_full, e_full, part,
    tot_buf, tot_own, ms_buf, ms_own, s_own, s_peer, t_chip, s_chips, p_own, p_peer,
    q_send, q_recv, kv_send, kv_recv, fwd_send,
    tot_send, tot_recv, ms_send, ms_recv, a_send, a_recv, b_send, b_recv, c_send, c_recv,
    rel_k, rel_v, rel_q, rel_send, rel_recv,
):
    me = lax.axis_index("seq")
    mz = lax.axis_index("head")
    core = lax.rem(me, 2)
    chip = me // 2
    chips = n // 2
    peer = me + 1 - 2 * core
    blk = q_ref.shape[1]
    feats = q_ref.shape[2]
    kv_local = k_ref.shape[2] // HDIM
    group = feats // HDIM // kv_local
    gcols = group * HDIM
    toks = 2 * blk
    heads = step_ref.shape[0]
    sdim = feats // heads
    tiles = feats // LANES
    half = feats // 2
    htiles = tiles // 2

    barrier = pltpu.get_barrier_semaphore()

    @pl.loop(1, n)
    def _(off):
        pl.semaphore_signal(
            barrier, inc=1, device_id={"seq": lax.rem(me + off, n)}, device_id_type=MESH
        )

    @pl.loop(1, nh)
    def _(off):
        pl.semaphore_signal(
            barrier, inc=1, device_id={"head": lax.rem(mz + off, nh)}, device_id_type=MESH
        )

    pl.semaphore_wait(barrier, n + nh - 2)

    quarter = n // 4

    def crosses(s):
        goal = quarter * s + chip // 2
        via = 2 * (2 * (goal // 2) + lax.rem(chip, 2)) + core
        return (lax.rem(goal, 2) != lax.rem(chip, 2)) & (goal // 2 != chip // 2), via

    goal_chip = 2 * (chip // 2) + 1 - lax.rem(chip, 2)
    relaying = lax.rem(goal_chip, quarter) != chip // 2
    goal = 2 * goal_chip + lax.rem(chip, 2)

    def pieces(g):
        return [pl.ds(g * gcols + j * HDIM, HDIM) for j in range(group)]

    def relay(g):
        kcols = pl.ds(g * HDIM, HDIM)
        rows = pl.ds(core * blk, blk)
        krows = pl.ds((2 + core) * blk, blk)
        return (
            (rel_k.at[:, kcols], k_buf.at[krows, kcols], 0, kv_recv.at[g, 2 + core, 0]),
            (rel_v.at[:, kcols], v_buf.at[krows, kcols], 1, kv_recv.at[g, 2 + core, 1]),
        ) + tuple(
            (rel_q.at[:, cols], q_buf.at[rows, cols], 2 + j, q_recv.at[g, core])
            for j, cols in enumerate(pieces(g))
        )

    def pass_on(g):
        @pl.when(relaying)
        def _():
            for held, dst, t, rsem in relay(g):
                arrived(held, rel_recv.at[g, t])
                remote(held, dst, rel_send.at[g, t], rsem, seq=goal).start()

    def moves(g):
        found = []
        for s in range(2):
            home = (n // 2) * s + chip
            diag, via = crosses(s)
            straight = jnp.logical_not(diag)
            kcols = pl.ds(g * HDIM, HDIM)
            qcols = pl.ds(g * gcols, gcols)
            for t, (src, dst) in enumerate(((k_ref, k_buf), (v_ref, v_buf))):
                found.append((
                    src.at[s, :, kcols],
                    dst.at[pl.ds((2 + core) * blk, blk), kcols],
                    kv_send.at[g, s, 0, t], kv_recv.at[g, 2 + core, t], home, straight,
                ))
                found.append((
                    src.at[s, :, kcols], (rel_k, rel_v)[t].at[:, kcols],
                    kv_send.at[g, s, 0, t], rel_recv.at[g, t], via, diag,
                ))
                found.append((
                    src.at[s, :, kcols],
                    dst.at[pl.ds(core * blk, blk), kcols],
                    kv_send.at[g, s, 1, t], kv_recv.at[g, core, t], home + 1,
                    (lax.rem(home, 2) == 1) & (home + 1 < n),
                ))
            found.append((
                q_ref.at[s, :, qcols],
                q_buf.at[pl.ds(core * blk, blk), qcols],
                q_send.at[g, s, 0], q_recv.at[g, core], home, straight,
            ))
            for j, cols in enumerate(pieces(g)):
                found.append((
                    q_ref.at[s, :, cols], rel_q.at[:, cols],
                    q_send.at[g, s, j], rel_recv.at[g, 2 + j], via, diag,
                ))
        return found

    def away(dest, cond):
        other = dest != me
        return other if cond is None else other & cond

    for g in range(kv_local):
        for src, dst, ssem, rsem, dest, cond in moves(g):

            @pl.when(away(dest, cond))
            def _():
                remote(src, dst, ssem, rsem, seq=dest).start()

            here = dest == me
            here = here if cond is None else here & cond

            @pl.when(here)
            def _():
                pltpu.make_async_copy(src, dst, rsem).start()

    @pl.when(me == 0)
    def _():
        k_buf[0:toks] = jnp.zeros_like(k_buf[0:toks])
        v_buf[0:toks] = jnp.zeros_like(v_buf[0:toks])

    t_ids = lax.broadcasted_iota(jnp.int32, (toks, toks), 0)
    u_ids = lax.broadcasted_iota(jnp.int32, (toks, toks), 1)
    upper = (t_ids <= u_ids).astype(F32)
    cum = dot(decay_ref[...], upper, ((1,), (0,)), lax.Precision.HIGHEST)
    cum_buf[...] = cum
    pick = (
        lax.broadcasted_iota(jnp.int32, (heads, feats), 1) // sdim
        == lax.broadcasted_iota(jnp.int32, (heads, feats), 0)
    ).astype(F32)
    total = jnp.sum(decay_ref[...], axis=1, keepdims=True)
    tot_row = jnp.sum(total * pick, axis=0, keepdims=True)
    for p in range(tiles):
        tot_own[p : p + 1, :] = tot_row[:, p * LANES : (p + 1) * LANES]

    def tot_copy(dest, source):
        return remote(
            tot_own, tot_buf.at[source], tot_send.at[dest], tot_recv.at[source], seq=dest
        )

    @pl.loop(1, n)
    def _(off):
        tot_copy(lax.rem(me + off, n), me).start()

    tot_buf[me] = tot_own[...]

    def expand(rows):
        high = rows.astype(BF16)
        low = (rows - high.astype(F32)).astype(BF16)
        both = jnp.concatenate([high, low], 0)
        pick2 = jnp.concatenate([pick, pick], 0).astype(BF16)
        return dot(both, pick2, ((0,), (0,)))

    w_full[...] = expand(jnp.exp(cum[:, toks - 1 : toks] - cum) * step_ref[...])
    e_full[...] = expand(jnp.exp(cum))
    cross = dot(c_ref[...], b_ref[...], ((1,), (1,)))
    part[:, 0:toks] = jnp.where(t_ids >= u_ids, cross, 0.0)

    def mix_head(h):
        row = cum_buf[pl.ds(h, 1), :]
        col = jnp.transpose(jnp.broadcast_to(row, (LANES, toks)))
        srow = step_ref[pl.ds(h, 1), :]
        for lo in range(0, toks, LANES):
            cols = slice(lo, lo + LANES)
            diff = jnp.minimum(col - row[:, cols], 0.0)
            mix[h, :, cols] = (jnp.exp(diff) * part[:, cols] * srow[:, cols]).astype(BF16)

    per = heads // kv_local
    for g in range(kv_local):
        pl.loop(g * per, (g + 1) * per)(mix_head)
        if g == 0:
            pass_on(g)

    factor = math.log2(math.e) / math.sqrt(HDIM)
    r_ids = lax.broadcasted_iota(jnp.int32, (blk, blk), 0)
    c_ids = lax.broadcasted_iota(jnp.int32, (blk, blk), 1)
    sumsq[...] = jnp.zeros_like(sumsq)
    for g in range(kv_local):
        if g > 0:
            pass_on(g)
        kcols = slice(g * HDIM, (g + 1) * HDIM)
        for slot in (2, 3):
            for t, buf in enumerate((k_buf, v_buf)):
                arrived(
                    buf.at[pl.ds(slot * blk, blk), pl.ds(g * HDIM, HDIM)],
                    kv_recv.at[g, slot, t],
                )

        @pl.when(core == 0)
        def _():
            for slot in (2, 3):
                for t, buf in enumerate((k_buf, v_buf)):
                    remote(
                        buf.at[pl.ds(slot * blk, blk), pl.ds(g * HDIM, HDIM)],
                        buf.at[pl.ds((slot - 2) * blk, blk), pl.ds(g * HDIM, HDIM)],
                        fwd_send.at[g, slot - 2, t], kv_recv.at[g, slot - 2, t], seq=peer,
                    ).start()

        @pl.when(me > 0)
        def _():
            for slot in (0, 1):
                for t, buf in enumerate((k_buf, v_buf)):
                    arrived(
                        buf.at[pl.ds(slot * blk, blk), pl.ds(g * HDIM, HDIM)],
                        kv_recv.at[g, slot, t],
                    )

        for slot in (0, 1):
            arrived(
                q_buf.at[pl.ds(slot * blk, blk), pl.ds(g * gcols, gcols)], q_recv.at[g, slot]
            )

        @pl.loop(0, group, unroll=2)
        def _(j):
            hcols = pl.ds(pl.multiple_of(g * gcols + j * HDIM, HDIM), HDIM)
            for slot in (0, 1):
                rows = slice(slot * blk, (slot + 1) * blk)
                keys = slice(slot * blk, (slot + 3) * blk)
                score = dot(q_buf[rows, hcols], k_buf[keys, kcols], ((1,), (1,)))
                far = (c_ids > r_ids) & (me > 0)
                mid = None if slot else jnp.broadcast_to(me > 0, (blk, blk))
                s0 = jnp.where(far, score[:, 0:blk], -jnp.inf)
                s1 = score[:, blk : 2 * blk]
                if slot == 0:
                    s1 = jnp.where(mid, s1, -jnp.inf)
                s2 = jnp.where(c_ids <= r_ids, score[:, 2 * blk :], -jnp.inf)
                peak = jnp.max(jnp.maximum(jnp.maximum(s0, s1), s2), axis=1, keepdims=True)
                e0 = jnp.exp2((s0 - peak) * factor)
                e1 = jnp.exp2((s1 - peak) * factor)
                e2 = jnp.exp2((s2 - peak) * factor)
                weight = jnp.concatenate([e0, e1, e2], 1).astype(BF16)
                whole = jnp.sum(e0 + e1 + e2, axis=1, keepdims=True)
                result = dot(weight, v_buf[keys, kcols], ((1,), (0,))) / whole
                result = result.astype(BF16)
                att[rows, hcols] = result
                wide = result.astype(F32)
                sumsq[rows, :] += wide * wide

    ms_row = jnp.sum(jnp.transpose(sumsq[...]), axis=0, keepdims=True)
    ms_own[...] = jnp.broadcast_to(ms_row, ms_own.shape)

    def ms_copy(dest, source):
        return remote(
            ms_own, ms_buf.at[source], ms_send.at[dest], ms_recv.at[source], head=dest
        )

    @pl.loop(1, nh)
    def _(off):
        ms_copy(lax.rem(mz + off, nh), mz).start()

    ms_buf[mz] = ms_own[...]

    @pl.loop(1, nh)
    def _(off):
        arrived(ms_buf.at[lax.rem(mz + off, nh)], ms_recv.at[lax.rem(mz + off, nh)])

    meansq = jnp.sum(ms_buf[...], axis=0)[0:1, :] * (1.0 / (feats * nh))
    scale = jnp.transpose(jnp.broadcast_to(lax.rsqrt(meansq + 1e-06), (LANES, toks)))

    b_turned = jnp.transpose(b_ref[...].astype(F32)).astype(BF16)
    for p in range(tiles):
        cols = slice(p * LANES, (p + 1) * LANES)
        normed = (att[:, cols].astype(F32) * gain_ref[:, cols] * scale).astype(BF16)
        att[:, cols] = normed
        scaled = (normed.astype(F32) * w_full[:, cols]).astype(BF16)
        into = slice((p % htiles) * LANES, (p % htiles + 1) * LANES)
        s_own[p // htiles, :, into] = dot(b_turned, scaled, ((1,), (0,))).astype(BF16)

    a_copy = remote(s_own, s_peer, a_send, a_recv, seq=peer)
    a_copy.start()

    @pl.loop(1, n)
    def _(off):
        arrived(tot_buf.at[lax.rem(me + off, n)], tot_recv.at[lax.rem(me + off, n)])

    def row_of(device, side):
        return jnp.concatenate(
            [tot_buf[device, pl.ds(side * htiles + q, 1), :] for q in range(htiles)], 1
        )

    even = core == 0
    one = jnp.ones((1, half), F32)
    mine_scale = jnp.where(even, jnp.exp(row_of(peer, core)), one)
    peer_scale = jnp.where(even, one, jnp.exp(row_of(me, core)))
    a_copy.wait_recv()
    t_chip[...] = (
        mine_scale * s_own[core].astype(F32) + peer_scale * s_peer[core].astype(F32)
    ).astype(BF16)

    def b_copy(dest, source):
        return remote(
            t_chip, s_chips.at[source], b_send.at[dest], b_recv.at[source],
            seq=2 * dest + core,
        )

    @pl.loop(chip + 1, chips)
    def _(dest):
        b_copy(dest, chip).start()

    left = lax.broadcasted_iota(jnp.int32, (toks, LANES), 1) < sdim
    skip_row = dot(skip_ref[...], pick, ((1,), (0,)), lax.Precision.HIGHEST)
    for p in range(tiles):
        cols = slice(p * LANES, (p + 1) * LANES)
        x = att[:, cols]
        zero = jnp.zeros_like(x)
        y = dot(mix[2 * p], jnp.where(left, x, zero), ((1,), (0,)))
        y += dot(mix[2 * p + 1], jnp.where(left, zero, x), ((1,), (0,)))
        part[:, cols] = y + skip_row[:, cols] * x.astype(F32)

    w_full[0 : s_own.shape[1], 0:half] = jnp.zeros((s_own.shape[1], half), F32)
    state = w_full.at[0 : s_own.shape[1], 0:half]

    @pl.loop(0, chip)
    def _(source):
        arrived(s_chips.at[source], b_recv.at[source])
        decay = jnp.exp(row_of(2 * source, core) + row_of(2 * source + 1, core))
        state[...] = decay * state[...] + s_chips[source].astype(F32)

    p_own[...] = state[...].astype(BF16)
    c_copy = remote(p_own, p_peer, c_send, c_recv, seq=peer)
    c_copy.start()

    def finish(side, entered):
        lanes = slice(side * half, (side + 1) * half)
        keep = jnp.where(even, one, jnp.exp(row_of(peer, side)))
        add = jnp.where(even, jnp.zeros_like(one), one)
        entering = keep * entered.astype(F32) + add * s_peer[side].astype(F32)
        term = dot(c_ref[...], entering.astype(BF16), ((1,), (0,)))
        out_ref[:, lanes] = (part[:, lanes] + term * e_full[:, lanes]).astype(BF16)

    c_copy.wait_recv()
    for side in range(2):
        finish(side, jnp.where(core == side, p_own[...], p_peer[...]))

    for g in range(kv_local):
        for src, dst, ssem, rsem, dest, cond in moves(g):

            @pl.when(away(dest, cond))
            def _():
                remote(src, dst, ssem, rsem, seq=dest).wait_send()

        @pl.when(relaying)
        def _():
            for held, dst, t, rsem in relay(g):
                remote(held, dst, rel_send.at[g, t], rsem, seq=goal).wait_send()

        @pl.when(core == 0)
        def _():
            for slot in (2, 3):
                for t, buf in enumerate((k_buf, v_buf)):
                    remote(
                        buf.at[pl.ds(slot * blk, blk), pl.ds(g * HDIM, HDIM)],
                        buf.at[pl.ds((slot - 2) * blk, blk), pl.ds(g * HDIM, HDIM)],
                        fwd_send.at[g, slot - 2, t], kv_recv.at[g, slot - 2, t], seq=peer,
                    ).wait_send()

    @pl.loop(1, n)
    def _(off):
        tot_copy(lax.rem(me + off, n), me).wait_send()

    @pl.loop(1, nh)
    def _(off):
        ms_copy(lax.rem(mz + off, nh), mz).wait_send()

    @pl.loop(chip + 1, chips)
    def _(dest):
        b_copy(dest, chip).wait_send()

    a_copy.wait_send()
    c_copy.wait_send()


def body(query, keys, values, norm_gain, in_b, out_c, step, log_decay, skip):
    n = lax.axis_size("seq")
    nh = lax.axis_size("head")
    blk, feats = query.shape[1], query.shape[2]
    kvcols = keys.shape[2]
    kv_local = kvcols // HDIM
    toks = 2 * blk
    heads = step.shape[0]
    nstate = in_b.shape[1]
    tiles = feats // LANES
    group = tiles // kv_local
    half = feats // 2
    chips = n // 2
    dma = pltpu.SemaphoreType.DMA
    vmem = pl.BlockSpec(memory_space=pltpu.VMEM)
    return pl.pallas_call(
        functools.partial(kernel, n, nh),
        out_shape=jax.ShapeDtypeStruct((toks, feats), BF16),
        in_specs=[vmem] * 9,
        out_specs=vmem,
        scratch_shapes=[
            pltpu.VMEM((toks, feats), BF16),
            pltpu.VMEM((2 * toks, kvcols), BF16),
            pltpu.VMEM((2 * toks, kvcols), BF16),
            pltpu.VMEM((toks, feats), BF16),
            pltpu.VMEM((toks, LANES), F32),
            pltpu.VMEM((heads, toks, toks), BF16),
            pltpu.VMEM((heads, toks), F32),
            pltpu.VMEM((toks, feats), F32),
            pltpu.VMEM((toks, feats), F32),
            pltpu.VMEM((toks, feats), F32),
            pltpu.VMEM((n, tiles, LANES), F32),
            pltpu.VMEM((tiles, LANES), F32),
            pltpu.VMEM((nh, 8, toks), F32),
            pltpu.VMEM((8, toks), F32),
            pltpu.VMEM((2, nstate, half), BF16),
            pltpu.VMEM((2, nstate, half), BF16),
            pltpu.VMEM((nstate, half), BF16),
            pltpu.VMEM((chips, nstate, half), BF16),
            pltpu.VMEM((nstate, half), BF16),
            pltpu.VMEM((nstate, half), BF16),
            dma((kv_local, 2, group)), dma((kv_local, 2)),
            dma((kv_local, 2, 2, 2)), dma((kv_local, 4, 2)), dma((kv_local, 2, 2)),
            dma((n,)), dma((n,)), dma((nh,)), dma((nh,)),
            dma, dma, dma((chips,)), dma((chips,)), dma, dma,
            pltpu.VMEM((blk, kvcols), BF16),
            pltpu.VMEM((blk, kvcols), BF16),
            pltpu.VMEM((blk, feats), BF16),
            dma((kv_local, 2 + group)), dma((kv_local, 2 + group)),
        ],
        compiler_params=pltpu.CompilerParams(
            collective_id=0, has_side_effects=True, vmem_limit_bytes=60 * 2**20
        ),
    )(
        query, keys, values, norm_gain.reshape(1, feats), in_b, out_c, step, log_decay,
        skip.reshape(1, heads),
    )


def solution(mesh):
    placed = (
        P(None, "seq", "head"),
        P(None, "seq", "head"),
        P(None, "seq", "head"),
        P("head"),
        P("seq", None),
        P("seq", None),
        P("head", "seq"),
        P("head", "seq"),
        P("head"),
    )
    return jax.shard_map(
        body, mesh=mesh, in_specs=placed, out_specs=P("seq", "head"), check_vma=False
    )
```
